32 devices in a mesh: blk: 8 (over z, x), shard: 4 (over y, core).
Axes of the slice: x: 2, y: 2, z: 4, core: 2. Of those that a mesh axis runs over, the one named last changes fastest.
Arguments:
- tokens: bfloat16 [8192, 2048], P(('blk', 'shard')), may hold values from -6 to 6
- targets: bfloat16 [8192, 2048], P(('blk', 'shard')), may hold values from -6 to 6
- up_weight: bfloat16 [2048, 7168], P(None, 'shard'), may hold values from -0.125 to 0.125
- down_weight: bfloat16 [8, 7168, 2048], P('blk', 'shard'), may hold values from -6 to 6
- mix_numer: int32 [2, 8, 3], replicated, may hold values from 1 to 2, as said below
Outputs:
- drift: bfloat16 [8, 7168, 2048], P('blk', 'shard')
The draws below stay inside these ranges and needn't reach their ends.
Inputs may be any that keep to these rules, and one draw needn't show every extreme that they name: Each row of mix_numer is (2, 1, 1), (1, 2, 1) or (1, 1, 2).
All inputs are finite; a program needn't handle non-finite values.
Results may differ from the reference program's by a relative error of at most 0.017.
Values may be sent and summed in bfloat16 or wider, within the bound.
No kernel may reach another device: no remote copies, remote signals or barrier semaphores. Data moves between devices by JAX's collectives and lax.ppermute only.
A program may use at most 128 MiB of HBM per device.

```python
import jax
import jax.numpy as jnp
from jax import lax

D = 2048
FF = 7168
TOK = 1024
ROUNDS = 2
NW = 8


def draw_mix_numer(key, part):
    picked = jax.random.randint(key, (ROUNDS, NW), 0, 3)
    return (1 + (picked[:, :, None] == jnp.arange(3, dtype=jnp.int32)[None, None, :]).astype(jnp.int32)).astype(jnp.int32)


def levels(key, shape, shards, low, high):
    factor_of = 1.0
    for axis_at, shards_of in shards:
        steps = jax.random.uniform(jax.random.fold_in(jax.random.fold_in(key, 6), axis_at), (shards_of,), jnp.float32, low / len(shards), high / len(shards))
        factor_of = factor_of * jnp.repeat(jnp.exp(steps), shape[axis_at] // shards_of).reshape((-1,) + (1,) * (len(shape) - 1 - axis_at))
    return factor_of


def noise(rng, shape, spread, limit, cuts=(), kind=jnp.bfloat16):
    result = jax.random.normal(rng, shape, jnp.float32) * spread
    if len(cuts) > 0:
        result = levels(rng, shape, cuts, -0.22, 0.18) * result
    return jnp.clip(result, min=-limit, max=limit).astype(kind)


def setup_inputs(seed: int = 0) -> dict:
    key_list = jax.random.split(jax.random.key(seed), 6)
    tokens = noise(key_list[0], (NW * TOK, D), 1.0, 6.0, ((0, 32),))
    targets = noise(key_list[1], (NW * TOK, D), 1.0, 6.0, ((0, 32),))
    up_weight = noise(key_list[2], (D, FF), D ** -0.5, 0.125, ((1, 4),))
    down_weight = noise(key_list[3], (NW, FF, D), 1.0, 6.0, ((0, 8), (1, 4)))
    mix_numer = draw_mix_numer(jax.random.fold_in(key_list[5], 71), 0)
    return {"tokens": tokens, "targets": targets, "up_weight": up_weight, "down_weight": down_weight, "mix_numer": mix_numer}


learn_rate = 2.0

def local_step(inputs, wanted, up_weight, weight):
    hidden = jax.nn.silu(jnp.dot(inputs, up_weight, preferred_element_type=jnp.float32)).astype(jnp.bfloat16)
    output = jnp.dot(hidden, weight, preferred_element_type=jnp.float32) / jnp.sqrt(jnp.float32(FF))
    resid = (output - wanted.astype(jnp.float32)).astype(jnp.bfloat16)
    grad = jnp.dot(hidden.T, resid, preferred_element_type=jnp.float32)
    return (weight.astype(jnp.float32) - learn_rate * grad / jnp.sqrt(jnp.float32(FF))).astype(jnp.bfloat16)

def mix_round(params, numer):

    def one(index):
        left_index = (index - 1) % NW
        right_index = (index + 1) % NW
        weights = numer[index].astype(jnp.float32)
        total = weights[0] * params[index].astype(jnp.float32) + weights[1] * params[left_index].astype(jnp.float32) + weights[2] * params[right_index].astype(jnp.float32)
        return (total / 4.0).astype(jnp.bfloat16)
    return lax.map(one, jnp.arange(NW, dtype=jnp.int32))

def reference(tokens, targets, up_weight, down_weight, mix_numer):
    inputs = tokens.reshape(NW, TOK, D)
    wanted = targets.reshape(NW, TOK, D)
    stepped = lax.map(lambda item: local_step(item[0], item[1], up_weight, item[2]), (inputs, wanted, down_weight))
    mixed = stepped
    for round_index in range(ROUNDS):
        mixed = mix_round(mixed, mix_numer[round_index])

    def accumulate(index, total):
        return total + mixed[index].astype(jnp.float32)
    total = lax.fori_loop(0, NW, accumulate, jnp.zeros((FF, D), jnp.float32))
    average = total / jnp.float32(NW)
    return lax.map(lambda item: (item.astype(jnp.float32) - average).astype(jnp.bfloat16), mixed)
```

```python
import functools

import jax
import jax.numpy as jnp
from jax import lax
from jax.experimental import pallas as pl
from jax.experimental.pallas import tpu as pltpu
from jax.sharding import PartitionSpec as P


learn_rate = 2.0
CUTS = (1, 2, 2, 2, 1)


def shifted(x, axis, by):
    devices = lax.axis_size(axis)
    return lax.ppermute(x, axis, [(i, (i + by) % devices) for i in range(devices)])


def other_core(x):
    devices = lax.axis_size("shard")
    return lax.ppermute(x, "shard", [(i, i ^ 1) for i in range(devices)])


def mix_kernel(rounds, workers, weights_ref, *refs):
    mixed = [ref[...].astype(jnp.float32) for ref in refs[:workers]]
    for r in range(rounds):
        mixed = [
            (
                weights_ref[r, j, 0] * mixed[j]
                + weights_ref[r, j, 1] * mixed[(j + 1) % workers]
                + weights_ref[r, j, 2] * mixed[(j - 1) % workers]
            )
            .astype(jnp.bfloat16)
            .astype(jnp.float32)
            for j in range(workers)
        ]
    total = mixed[0]
    for m in mixed[1:]:
        total = total + m
    average = total * (1.0 / workers)
    for j in range(workers):
        refs[workers + j][...] = (mixed[j] - average).astype(jnp.bfloat16)


def mix_blocks(blocks, weights):
    workers = len(blocks)
    rows, width = blocks[0].shape
    tile = next(t for t in (32, 16, 8) if rows % t == 0)
    spec = pl.BlockSpec((tile, width), lambda i: (i, 0))
    return pl.pallas_call(
        functools.partial(mix_kernel, weights.shape[0], workers),
        grid=(rows // tile,),
        in_specs=[pl.BlockSpec(memory_space=pltpu.SMEM)] + [spec] * workers,
        out_specs=[spec] * workers,
        out_shape=[jax.ShapeDtypeStruct((rows, width), jnp.bfloat16)] * workers,
        cost_estimate=pl.CostEstimate(
            flops=20 * workers * rows * width,
            bytes_accessed=4 * workers * rows * width,
            transcendentals=0,
        ),
        name="mix_blocks",
    )(weights, *blocks)


def body(tokens, targets, up_weight, down_weight, mix_numer):
    weight = down_weight[0]
    units, width = weight.shape
    workers = lax.axis_size("blk")
    me = lax.axis_index("blk")
    shards = lax.axis_size("shard")
    chips = shards // 2
    rows = tokens.shape[0]
    block = units // workers
    out_scale = 1.0 / jnp.sqrt(jnp.float32(units * shards))

    def hidden_of(x):
        return jax.nn.silu(jnp.dot(x, up_weight, preferred_element_type=jnp.float32)).astype(jnp.bfloat16)

    mine = [tokens] + [shifted(tokens, "shard", -2 * d) for d in range(1, chips)]
    hidden = jnp.concatenate(
        [hidden_of(jnp.concatenate([x, other_core(x)], axis=0)) for x in mine], axis=0
    )

    order = (me - jnp.arange(workers)) % workers
    weights = jnp.take(mix_numer, order, axis=1).astype(jnp.float32) * 0.25

    unit = width // sum(CUTS)
    result = jnp.zeros((workers, block, width), jnp.bfloat16)
    begin = 0
    for cut in CUTS:
        step = cut * unit
        cols = slice(begin, begin + step)
        part = weight[:, cols]
        output = jnp.dot(hidden, part, preferred_element_type=jnp.float32) * out_scale
        output = output.reshape(chips, 2, rows, step)
        summed = output[:, 0] + other_core(output[:, 1].astype(jnp.bfloat16)).astype(jnp.float32)
        summed = summed.at[0].add(-targets[:, cols].astype(jnp.float32)).astype(jnp.bfloat16)
        total = summed.astype(jnp.float32)
        for d in range(1, chips):
            got = shifted(summed, "shard", -2 * d).astype(jnp.float32)
            total = total + jnp.roll(got, d, axis=0)
        resid = total.astype(jnp.bfloat16)
        resid = jnp.stack([resid, other_core(resid)], axis=1).reshape(shards * rows, step)
        grad = lax.dot_general(hidden, resid, (((0,), (0,)), ((), ())), preferred_element_type=jnp.float32)
        stepped = (part.astype(jnp.float32) - (learn_rate * out_scale) * grad).astype(jnp.bfloat16)
        stepped = stepped.reshape(workers, block, step)
        blocks = [
            shifted(lax.dynamic_index_in_dim(stepped, (me + j) % workers, 0, keepdims=False), "blk", j)
            if j
            else lax.dynamic_index_in_dim(stepped, me, 0, keepdims=False)
            for j in range(workers)
        ]
        drift = mix_blocks(blocks, weights)
        for j in range(workers):
            back = shifted(drift[j], "blk", -j) if j else drift[0]
            result = lax.dynamic_update_slice(result, back[None], ((me + j) % workers, 0, begin))
        begin += step
    return result.reshape(1, units, width)


def solution(mesh):
    in_specs = (P(("blk", "shard"), None), P(("blk", "shard"), None), P(None, "shard"), P("blk", "shard", None), P())
    return jax.shard_map(body, mesh=mesh, in_specs=in_specs, out_specs=P("blk", "shard", None), check_vma=False)
```

```python
import functools

import jax
import jax.numpy as jnp
from jax import lax
from jax.experimental import pallas as pl
from jax.experimental.pallas import tpu as pltpu
from jax.sharding import PartitionSpec as P


learn_rate = 2.0
CUTS = (2, 3, 4, 6, 1)


def shifted(x, axis, by):
    devices = lax.axis_size(axis)
    return lax.ppermute(x, axis, [(i, (i + by) % devices) for i in range(devices)])


def other_core(x):
    devices = lax.axis_size("shard")
    return lax.ppermute(x, "shard", [(i, i ^ 1) for i in range(devices)])


def mix_kernel(rounds, workers, weights_ref, *refs):
    mixed = [ref[...].astype(jnp.float32) for ref in refs[:workers]]
    for r in range(rounds):
        mixed = [
            (
                weights_ref[r, j, 0] * mixed[j]
                + weights_ref[r, j, 1] * mixed[(j + 1) % workers]
                + weights_ref[r, j, 2] * mixed[(j - 1) % workers]
            )
            .astype(jnp.bfloat16)
            .astype(jnp.float32)
            for j in range(workers)
        ]
    total = mixed[0]
    for m in mixed[1:]:
        total = total + m
    average = total * (1.0 / workers)
    for j in range(workers):
        refs[workers + j][...] = (mixed[j] - average).astype(jnp.bfloat16)


def mix_blocks(blocks, weights):
    workers = len(blocks)
    rows, width = blocks[0].shape
    tile = next(t for t in (32, 16, 8) if rows % t == 0)
    spec = pl.BlockSpec((tile, width), lambda i: (i, 0))
    return pl.pallas_call(
        functools.partial(mix_kernel, weights.shape[0], workers),
        grid=(rows // tile,),
        in_specs=[pl.BlockSpec(memory_space=pltpu.SMEM)] + [spec] * workers,
        out_specs=[spec] * workers,
        out_shape=[jax.ShapeDtypeStruct((rows, width), jnp.bfloat16)] * workers,
        cost_estimate=pl.CostEstimate(
            flops=20 * workers * rows * width,
            bytes_accessed=4 * workers * rows * width,
            transcendentals=0,
        ),
        name="mix_blocks",
    )(weights, *blocks)


def place_kernel(begin, *refs):
    blocks, result_ref, sems = refs[: -2], refs[-2], refs[-1]
    workers, _, _ = result_ref.shape
    blocks = blocks[:workers]
    me = lax.axis_index("blk")
    copies = []
    for j in range(workers):
        target = result_ref.at[lax.rem(me + j, workers), :, pl.ds(begin, blocks[j].shape[1])]
        copies.append(pltpu.make_async_copy(blocks[j], target, sems.at[j]))
    for copy in copies:
        copy.start()
    for copy in copies:
        copy.wait()


def place_blocks(blocks, begin, shape, result):
    workers = len(blocks)
    inside = pl.BlockSpec(memory_space=pltpu.VMEM)
    outside = pl.BlockSpec(memory_space=pl.ANY)
    held = [] if result is None else [result]
    return pl.pallas_call(
        functools.partial(place_kernel, begin),
        in_specs=[inside] * workers + [outside] * len(held),
        out_specs=outside,
        out_shape=jax.ShapeDtypeStruct(shape, jnp.bfloat16),
        scratch_shapes=[pltpu.SemaphoreType.DMA((workers,))],
        input_output_aliases={workers: 0} if held else {},
        cost_estimate=pl.CostEstimate(
            flops=4 * blocks[0].size * workers, bytes_accessed=4 * blocks[0].size * workers, transcendentals=0
        ),
        name="place_blocks",
    )(*blocks, *held)


def body(tokens, targets, up_weight, down_weight, mix_numer):
    weight = down_weight[0]
    units, width = weight.shape
    workers = lax.axis_size("blk")
    me = lax.axis_index("blk")
    shards = lax.axis_size("shard")
    chips = shards // 2
    rows = tokens.shape[0]
    block = units // workers
    out_scale = 1.0 / jnp.sqrt(jnp.float32(units * shards))
    parts = len(CUTS)

    mine = [tokens] + [shifted(tokens, "shard", -2 * d) for d in range(1, chips)]
    hidden = []
    for x in mine:
        x = jnp.concatenate([x, other_core(x)], axis=0)
        hidden.append(
            jax.nn.silu(jnp.dot(x, up_weight, preferred_element_type=jnp.float32)).astype(jnp.bfloat16)
        )
    hidden = jnp.concatenate(hidden, axis=0)

    order = (me - jnp.arange(workers)) % workers
    weights = jnp.take(mix_numer, order, axis=1).astype(jnp.float32) * 0.25

    unit = width // sum(CUTS)
    begins = [unit * sum(CUTS[:c]) for c in range(parts)]
    arrived = []
    for c in range(parts):
        step = unit * CUTS[c]
        cols = slice(begins[c], begins[c] + step)
        part = weight[:, cols]
        output = jnp.dot(hidden, part, preferred_element_type=jnp.float32) * out_scale
        output = output.reshape(chips, 2, rows, step)
        summed = output[:, 0] + other_core(output[:, 1].astype(jnp.bfloat16)).astype(jnp.float32)
        summed = summed.at[0].add(-targets[:, cols].astype(jnp.float32)).astype(jnp.bfloat16)
        total = summed.astype(jnp.float32)
        for d in range(1, chips):
            got = shifted(summed, "shard", -2 * d).astype(jnp.float32)
            total = total + jnp.roll(got, d, axis=0)
        resid = total.astype(jnp.bfloat16)
        resid = jnp.stack([resid, other_core(resid)], axis=1).reshape(shards * rows, step)
        grad = lax.dot_general(hidden, resid, (((0,), (0,)), ((), ())), preferred_element_type=jnp.float32)
        stepped = (part.astype(jnp.float32) - (learn_rate * out_scale) * grad).astype(jnp.bfloat16)
        stepped = stepped.reshape(workers, block, step)
        blocks = [lax.dynamic_index_in_dim(stepped, (me + j) % workers, 0, keepdims=False) for j in range(workers)]
        arrived.append([shifted(x, "blk", j) if j else x for j, x in enumerate(blocks)])
    returned = []
    for c in range(parts):
        drift = mix_blocks(arrived[c], weights)
        returned.append([shifted(x, "blk", -j) if j else x for j, x in enumerate(drift)])
    result = None
    for c in range(parts):
        result = place_blocks(returned[c], begins[c], (workers, block, width), result)
    return result.reshape(1, units, width)


def solution(mesh):
    in_specs = (P(("blk", "shard"), None), P(("blk", "shard"), None), P(None, "shard"), P("blk", "shard", None), P())

    return jax.shard_map(body, mesh=mesh, in_specs=in_specs, out_specs=P("blk", "shard", None), check_vma=False)
```

```python
import functools

import jax
import jax.numpy as jnp
from jax import lax
from jax.experimental import pallas as pl
from jax.experimental.pallas import tpu as pltpu
from jax.sharding import PartitionSpec as P


learn_rate = 2.0
VMEM_LIMIT = 16 * 1024 * 1024
CUTS = (2, 4, 6, 3, 1)


def shifted(x, axis, by):
    devices = lax.axis_size(axis)
    return lax.ppermute(x, axis, [(i, (i + by) % devices) for i in range(devices)])


def exchanged(blocks, sign):
    workers = len(blocks)
    moved = {}
    for j in sorted(range(1, workers), key=lambda j: abs(2 * j - workers)):
        moved[j] = shifted(blocks[j], "blk", sign * j)
    return [blocks[0]] + [moved[j] for j in range(1, workers)]


def other_core(x):
    devices = lax.axis_size("shard")
    return lax.ppermute(x, "shard", [(i, i ^ 1) for i in range(devices)])


def mix_kernel(rounds, workers, weights_ref, *refs):
    mixed = [ref[...].astype(jnp.float32) for ref in refs[:workers]]
    for r in range(rounds):
        mixed = [
            (
                weights_ref[r, j, 0] * mixed[j]
                + weights_ref[r, j, 1] * mixed[(j + 1) % workers]
                + weights_ref[r, j, 2] * mixed[(j - 1) % workers]
            )
            .astype(jnp.bfloat16)
            .astype(jnp.float32)
            for j in range(workers)
        ]
    total = mixed[0]
    for m in mixed[1:]:
        total = total + m
    average = total * (1.0 / workers)
    for j in range(workers):
        refs[workers + j][...] = (mixed[j] - average).astype(jnp.bfloat16)


def mix_blocks(blocks, weights):
    workers = len(blocks)
    rows, width = blocks[0].shape
    tile = next(t for t in (32, 16, 8) if rows % t == 0)
    spec = pl.BlockSpec((tile, width), lambda i: (i, 0))
    return pl.pallas_call(
        functools.partial(mix_kernel, weights.shape[0], workers),
        grid=(rows // tile,),
        in_specs=[pl.BlockSpec(memory_space=pltpu.SMEM)] + [spec] * workers,
        out_specs=[spec] * workers,
        out_shape=[jax.ShapeDtypeStruct((rows, width), jnp.bfloat16)] * workers,
        cost_estimate=pl.CostEstimate(
            flops=20 * workers * rows * width,
            bytes_accessed=4 * workers * rows * width,
            transcendentals=0,
        ),
        compiler_params=pltpu.CompilerParams(vmem_limit_bytes=VMEM_LIMIT // 2),
        name="mix_blocks",
    )(weights, *blocks)


def place_kernel(begin, *refs):
    blocks, result_ref, sems = refs[: -2], refs[-2], refs[-1]
    workers, _, _ = result_ref.shape
    blocks = blocks[:workers]
    me = lax.axis_index("blk")
    copies = []
    for j in range(workers):
        target = result_ref.at[lax.rem(me + j, workers), :, pl.ds(begin, blocks[j].shape[1])]
        copies.append(pltpu.make_async_copy(blocks[j], target, sems.at[j]))
    for copy in copies:
        copy.start()
    for copy in copies:
        copy.wait()


def place_blocks(blocks, begin, shape, result):
    workers = len(blocks)
    inside = pl.BlockSpec(memory_space=pltpu.VMEM)
    outside = pl.BlockSpec(memory_space=pl.ANY)
    held = [] if result is None else [result]
    return pl.pallas_call(
        functools.partial(place_kernel, begin),
        in_specs=[inside] * workers + [outside] * len(held),
        out_specs=outside,
        out_shape=jax.ShapeDtypeStruct(shape, jnp.bfloat16),
        scratch_shapes=[pltpu.SemaphoreType.DMA((workers,))],
        input_output_aliases={workers: 0} if held else {},
        cost_estimate=pl.CostEstimate(
            flops=4 * blocks[0].size * workers, bytes_accessed=4 * blocks[0].size * workers, transcendentals=0
        ),
        compiler_params=pltpu.CompilerParams(vmem_limit_bytes=VMEM_LIMIT // 2),
        name="place_blocks",
    )(*blocks, *held)


def out_kernel(begin, scale, *refs):
    hidden_refs, (targets_ref, weight_ref, own_ref, other_ref, part_ref, sem) = refs[:-6], refs[-6:]
    _, step = own_ref.shape[1:]
    copy = pltpu.make_async_copy(weight_ref.at[:, pl.ds(begin, step)], part_ref, sem)
    copy.start()
    copy.wait()
    for d in range(own_ref.shape[0]):
        own, other = (
            jnp.dot(ref[...], part_ref[...], preferred_element_type=jnp.float32) * scale
            for ref in hidden_refs[2 * d : 2 * d + 2]
        )
        if d == 0:
            own = own - targets_ref[:, begin : begin + step].astype(jnp.float32)
        own_ref[d] = own
        other_ref[d] = other.astype(jnp.bfloat16)


def out_part(hidden, targets, weight, begin, step, scale):
    chips, rows = len(hidden) // 2, targets.shape[0]
    inside = pl.BlockSpec(memory_space=pltpu.VMEM)
    outside = pl.BlockSpec(memory_space=pl.ANY)
    units = weight.shape[0]
    return pl.pallas_call(
        functools.partial(out_kernel, begin, scale),
        in_specs=[inside] * (2 * chips + 1) + [outside],
        out_specs=[inside, inside],
        out_shape=[
            jax.ShapeDtypeStruct((chips, rows, step), jnp.float32),
            jax.ShapeDtypeStruct((chips, rows, step), jnp.bfloat16),
        ],
        scratch_shapes=[pltpu.VMEM((units, step), jnp.bfloat16), pltpu.SemaphoreType.DMA],
        compiler_params=pltpu.CompilerParams(vmem_limit_bytes=VMEM_LIMIT),
        cost_estimate=pl.CostEstimate(
            flops=4 * chips * rows * units * step, bytes_accessed=2 * units * step, transcendentals=0
        ),
        name="out_part",
    )(*hidden, targets, weight)


def grad_kernel(begin, scale, chips, unrolled, *refs):
    hidden_refs, refs = refs[: 2 * chips], refs[2 * chips :]
    resid_ref, other_ref, weight_ref = refs[:3]
    block_refs, (part_ref, stepped_ref, sem) = refs[3:-3], refs[-3:]
    workers = len(block_refs)
    step = resid_ref.shape[2]
    units = part_ref.shape[0]
    block = units // workers
    tile = next(t for t in (256, 128) if units % t == 0)
    copy = pltpu.make_async_copy(weight_ref.at[:, pl.ds(begin, step)], part_ref, sem)
    copy.start()

    def one_tile(i):
        at = pl.ds(i * tile if isinstance(i, int) else pl.multiple_of(i * tile, tile), tile)
        grad = None
        for piece, hidden_ref in enumerate(hidden_refs):
            term = lax.dot_general(
                hidden_ref[:, at],
                (resid_ref, other_ref)[piece % 2][piece // 2],
                (((0,), (0,)), ((), ())),
                preferred_element_type=jnp.float32,
            )
            grad = term if grad is None else grad + term
        pl.when(i == 0)(copy.wait)
        stepped_ref[at] = (part_ref[at].astype(jnp.float32) - scale * grad).astype(jnp.bfloat16)

    if unrolled:
        for i in range(units // tile):
            one_tile(i)
    else:
        pl.loop(0, units // tile)(one_tile)
    me = lax.axis_index("blk")
    for j in range(workers):
        first = pl.multiple_of(lax.rem(me + j, workers) * block, 8)
        block_refs[j][...] = stepped_ref[pl.ds(first, block), :]


def grad_part(hidden, resid, other, weight, begin, scale, workers, unrolled):
    chips, rows, step = resid.shape
    units = weight.shape[0]
    inside = pl.BlockSpec(memory_space=pltpu.VMEM)
    outside = pl.BlockSpec(memory_space=pl.ANY)
    return pl.pallas_call(
        functools.partial(grad_kernel, begin, scale, chips, unrolled),
        in_specs=[inside] * (2 * chips + 2) + [outside],
        out_specs=[inside] * workers,
        out_shape=[jax.ShapeDtypeStruct((units // workers, step), jnp.bfloat16)] * workers,
        scratch_shapes=[
            pltpu.VMEM((units, step), jnp.bfloat16),
            pltpu.VMEM((units, step), jnp.bfloat16),
            pltpu.SemaphoreType.DMA,
        ],
        compiler_params=pltpu.CompilerParams(vmem_limit_bytes=VMEM_LIMIT),
        cost_estimate=pl.CostEstimate(
            flops=4 * chips * rows * units * step, bytes_accessed=4 * units * step, transcendentals=0
        ),
        name="grad_part",
    )(*hidden, resid, other, weight)


def body(tokens, targets, up_weight, down_weight, mix_numer):
    weight = down_weight[0]
    units, width = weight.shape
    workers = lax.axis_size("blk")
    me = lax.axis_index("blk")
    shards = lax.axis_size("shard")
    chips = shards // 2
    block = units // workers
    out_scale = 1.0 / (units * shards) ** 0.5
    parts = len(CUTS)

    mine = [tokens] + [shifted(tokens, "shard", -2 * d) for d in range(1, chips)]
    hidden = []
    for x in mine:
        pair = (x, other_core(x))
        for x in pair:
            hidden.append(jax.nn.silu(jnp.dot(x, up_weight, preferred_element_type=jnp.float32)).astype(jnp.bfloat16))

    order = (me - jnp.arange(workers)) % workers
    weights = jnp.take(mix_numer, order, axis=1).astype(jnp.float32) * 0.25

    unit = width // sum(CUTS)
    begins = [unit * sum(CUTS[:c]) for c in range(parts)]
    arrived = []
    for c in range(parts):
        step = unit * CUTS[c]
        own, other = out_part(hidden, targets, weight, begins[c], step, out_scale)
        summed = (own + other_core(other).astype(jnp.float32)).astype(jnp.bfloat16)
        total = summed.astype(jnp.float32)
        for d in range(1, chips):
            got = shifted(summed, "shard", -2 * d).astype(jnp.float32)
            total = total + jnp.roll(got, d, axis=0)
        resid = total.astype(jnp.bfloat16)
        other = other_core(resid)
        blocks = grad_part(hidden, resid, other, weight, begins[c], learn_rate * out_scale, workers, c < 2)
        arrived.append(exchanged(blocks, 1))
    returned = []
    for c in range(parts):
        drift = mix_blocks(arrived[c], weights)
        returned.append(exchanged(drift, -1))
    result = None
    for c in range(parts):
        result = place_blocks(returned[c], begins[c], (workers, block, width), result)
    return result.reshape(1, units, width)


def solution(mesh):
    in_specs = (P(("blk", "shard"), None), P(("blk", "shard"), None), P(None, "shard"), P("blk", "shard", None), P())

    return jax.shard_map(body, mesh=mesh, in_specs=in_specs, out_specs=P("blk", "shard", None), check_vma=False)
```

```python
import functools

import jax
import jax.numpy as jnp
from jax import lax
from jax.experimental import pallas as pl
from jax.experimental.pallas import tpu as pltpu
from jax.sharding import PartitionSpec as P


learn_rate = 2.0
AHEAD = 3
VMEM_LIMIT = 16 * 1024 * 1024
CUTS = (2, 4, 5, 3, 2)


def shifted(x, axis, by):
    devices = lax.axis_size(axis)
    return lax.ppermute(x, axis, [(i, (i + by) % devices) for i in range(devices)])


def exchanged(blocks, sign):
    workers = len(blocks)
    moved = {}
    for j in sorted(range(1, workers), key=lambda j: abs(2 * j - workers)):
        moved[j] = shifted(blocks[j], "blk", sign * j)
    return [blocks[0]] + [moved[j] for j in range(1, workers)]


def other_core(x):
    devices = lax.axis_size("shard")
    return lax.ppermute(x, "shard", [(i, i ^ 1) for i in range(devices)])


def mix_kernel(rounds, workers, weights_ref, *refs):
    mixed = [ref[...].astype(jnp.float32) for ref in refs[:workers]]
    for r in range(rounds):
        mixed = [
            (
                weights_ref[r, j, 0] * mixed[j]
                + weights_ref[r, j, 1] * mixed[(j + 1) % workers]
                + weights_ref[r, j, 2] * mixed[(j - 1) % workers]
            )
            .astype(jnp.bfloat16)
            .astype(jnp.float32)
            for j in range(workers)
        ]
    total = mixed[0]
    for m in mixed[1:]:
        total = total + m
    average = total * (1.0 / workers)
    for j in range(workers):
        refs[workers + j][...] = (mixed[j] - average).astype(jnp.bfloat16)


def mix_blocks(blocks, weights):
    workers = len(blocks)
    rows, width = blocks[0].shape
    tile = next(t for t in (32, 16, 8) if rows % t == 0)
    spec = pl.BlockSpec((tile, width), lambda i: (i, 0))
    return pl.pallas_call(
        functools.partial(mix_kernel, weights.shape[0], workers),
        grid=(rows // tile,),
        in_specs=[pl.BlockSpec(memory_space=pltpu.SMEM)] + [spec] * workers,
        out_specs=[spec] * workers,
        out_shape=[jax.ShapeDtypeStruct((rows, width), jnp.bfloat16)] * workers,
        cost_estimate=pl.CostEstimate(
            flops=20 * workers * rows * width,
            bytes_accessed=4 * workers * rows * width,
            transcendentals=0,
        ),
        compiler_params=pltpu.CompilerParams(vmem_limit_bytes=VMEM_LIMIT // 2),
        name="mix_blocks",
    )(weights, *blocks)


def place_kernel(begin, *refs):
    blocks, result_ref, sems = refs[: -2], refs[-2], refs[-1]
    workers, _, _ = result_ref.shape
    blocks = blocks[:workers]
    me = lax.axis_index("blk")
    copies = []
    for j in range(workers):
        target = result_ref.at[lax.rem(me + j, workers), :, pl.ds(begin, blocks[j].shape[1])]
        copies.append(pltpu.make_async_copy(blocks[j], target, sems.at[j]))
    for copy in copies:
        copy.start()
    for copy in copies:
        copy.wait()


def place_blocks(blocks, begin, shape, result):
    workers = len(blocks)
    inside = pl.BlockSpec(memory_space=pltpu.VMEM)
    outside = pl.BlockSpec(memory_space=pl.ANY)
    held = [] if result is None else [result]
    return pl.pallas_call(
        functools.partial(place_kernel, begin),
        in_specs=[inside] * workers + [outside] * len(held),
        out_specs=outside,
        out_shape=jax.ShapeDtypeStruct(shape, jnp.bfloat16),
        scratch_shapes=[pltpu.SemaphoreType.DMA((workers,))],
        input_output_aliases={workers: 0} if held else {},
        cost_estimate=pl.CostEstimate(
            flops=4 * blocks[0].size * workers, bytes_accessed=4 * blocks[0].size * workers, transcendentals=0
        ),
        compiler_params=pltpu.CompilerParams(vmem_limit_bytes=VMEM_LIMIT // 2),
        name="place_blocks",
    )(*blocks, *held)


def out_kernel(begin, scale, *refs):
    weight_ref, own_ref, other_ref, part_ref, sem = refs[-5:]
    chips = own_ref.shape[0]
    hidden_refs, targets_refs = refs[: 2 * chips], refs[2 * chips : -5]
    step = own_ref.shape[2]
    copy = pltpu.make_async_copy(weight_ref.at[:, pl.ds(begin, step)], part_ref, sem)
    copy.start()
    copy.wait()
    for d in range(chips):
        own, other = (
            jnp.dot(ref[...], part_ref[...], preferred_element_type=jnp.float32) * scale
            for ref in hidden_refs[2 * d : 2 * d + 2]
        )
        if d == 0 and targets_refs:
            own = own - targets_refs[0][:, begin : begin + step].astype(jnp.float32)
        own_ref[d] = own
        other_ref[d] = other.astype(jnp.bfloat16)


def out_part(hidden, targets, weight, begin, step, scale):
    chips, rows = len(hidden) // 2, hidden[0].shape[0]
    inside = pl.BlockSpec(memory_space=pltpu.VMEM)
    outside = pl.BlockSpec(memory_space=pl.ANY)
    units = weight.shape[0]
    return pl.pallas_call(
        functools.partial(out_kernel, begin, scale),
        in_specs=[inside] * (2 * chips + len(targets)) + [outside],
        out_specs=[inside, inside],
        out_shape=[
            jax.ShapeDtypeStruct((chips, rows, step), jnp.float32),
            jax.ShapeDtypeStruct((chips, rows, step), jnp.bfloat16),
        ],
        scratch_shapes=[pltpu.VMEM((units, step), jnp.bfloat16), pltpu.SemaphoreType.DMA],
        compiler_params=pltpu.CompilerParams(vmem_limit_bytes=VMEM_LIMIT),
        cost_estimate=pl.CostEstimate(
            flops=4 * chips * rows * units * step, bytes_accessed=2 * units * step, transcendentals=0
        ),
        name="out_part",
    )(*hidden, *targets, weight)


def grad_kernel(begin, scale, chips, unrolled, *refs):
    hidden_refs, refs = refs[: 2 * chips], refs[2 * chips :]
    resid_ref, other_ref, weight_ref = refs[:3]
    block_refs, (part_ref, stepped_ref, sem) = refs[3:-3], refs[-3:]
    workers = len(block_refs)
    step = resid_ref.shape[2]
    units = part_ref.shape[0]
    block = units // workers
    tile = next(t for t in (256, 128) if units % t == 0)
    copy = pltpu.make_async_copy(weight_ref.at[:, pl.ds(begin, step)], part_ref, sem)
    copy.start()

    def one_tile(i):
        at = pl.ds(i * tile if isinstance(i, int) else pl.multiple_of(i * tile, tile), tile)
        grad = None
        for piece, hidden_ref in enumerate(hidden_refs):
            term = lax.dot_general(
                hidden_ref[:, at],
                (resid_ref, other_ref)[piece % 2][piece // 2],
                (((0,), (0,)), ((), ())),
                preferred_element_type=jnp.float32,
            )
            grad = term if grad is None else grad + term
        pl.when(i == 0)(copy.wait)
        stepped_ref[at] = (part_ref[at].astype(jnp.float32) - scale * grad).astype(jnp.bfloat16)

    if unrolled:
        for i in range(units // tile):
            one_tile(i)
    else:
        pl.loop(0, units // tile)(one_tile)
    me = lax.axis_index("blk")
    for j in range(workers):
        first = pl.multiple_of(lax.rem(me + j, workers) * block, 8)
        block_refs[j][...] = stepped_ref[pl.ds(first, block), :]


def grad_part(hidden, resid, other, weight, begin, scale, workers, unrolled):
    chips, rows, step = resid.shape
    units = weight.shape[0]
    inside = pl.BlockSpec(memory_space=pltpu.VMEM)
    outside = pl.BlockSpec(memory_space=pl.ANY)
    return pl.pallas_call(
        functools.partial(grad_kernel, begin, scale, chips, unrolled),
        in_specs=[inside] * (2 * chips + 2) + [outside],
        out_specs=[inside] * workers,
        out_shape=[jax.ShapeDtypeStruct((units // workers, step), jnp.bfloat16)] * workers,
        scratch_shapes=[
            pltpu.VMEM((units, step), jnp.bfloat16),
            pltpu.VMEM((units, step), jnp.bfloat16),
            pltpu.SemaphoreType.DMA,
        ],
        compiler_params=pltpu.CompilerParams(vmem_limit_bytes=VMEM_LIMIT),
        cost_estimate=pl.CostEstimate(
            flops=4 * chips * rows * units * step, bytes_accessed=4 * units * step, transcendentals=0
        ),
        name="grad_part",
    )(*hidden, resid, other, weight)


def body(tokens, targets, up_weight, down_weight, mix_numer):
    weight = down_weight[0]
    units, width = weight.shape
    workers = lax.axis_size("blk")
    me = lax.axis_index("blk")
    shards = lax.axis_size("shard")
    chips = shards // 2
    block = units // workers
    out_scale = 1.0 / (units * shards) ** 0.5
    parts = len(CUTS)

    mine = [tokens] + [shifted(tokens, "shard", -2 * d) for d in range(1, chips)]
    hidden = []
    for x in mine:
        pair = (x, other_core(x))
        for x in pair:
            hidden.append(jax.nn.silu(jnp.dot(x, up_weight, preferred_element_type=jnp.float32)).astype(jnp.bfloat16))

    order = (me - jnp.arange(workers)) % workers
    weights = jnp.take(mix_numer, order, axis=1).astype(jnp.float32) * 0.25

    unit = width // sum(CUTS)
    begins = [unit * sum(CUTS[:c]) for c in range(parts)]
    arrived = []
    for c in range(parts):
        step = unit * CUTS[c]
        runs = ((0, 1), (1, chips)) if c < AHEAD and chips > 1 else ((0, chips),)
        sums = []
        got = {}
        for first, last in runs:
            own, other = out_part(
                hidden[2 * first : 2 * last],
                [] if first else [targets],
                weight,
                begins[c],
                step,
                out_scale,
            )
            if sums:
                own, *sums = lax.optimization_barrier((own, *sums))
            summed = (own + other_core(other).astype(jnp.float32)).astype(jnp.bfloat16)
            sums += [summed[i] for i in range(last - first)]
            if c and last < chips:
                continue
            sent = summed if c == 0 or len(runs) == 1 else jnp.stack(sums)
            for d in range(1, chips):
                moved = shifted(sent, "shard", -2 * d)
                for i in range(sent.shape[0]):
                    got.setdefault((d + i + (first if c == 0 else 0)) % chips, []).append(moved[i])
        totals = [x.astype(jnp.float32) for x in sums]
        for n, terms in got.items():
            for x in terms:
                totals[n] = totals[n] + x.astype(jnp.float32)
        resid = jnp.stack(totals).astype(jnp.bfloat16)
        other = other_core(resid)
        blocks = grad_part(hidden, resid, other, weight, begins[c], learn_rate * out_scale, workers, c < 2)
        arrived.append(exchanged(blocks, 1))
    returned = []
    for c in range(parts):
        drift = mix_blocks(arrived[c], weights)
        returned.append(exchanged(drift, -1))
    result = None
    for c in range(parts):
        result = place_blocks(returned[c], begins[c], (workers, block, width), result)
    return result.reshape(1, units, width)


def solution(mesh):
    in_specs = (P(("blk", "shard"), None), P(("blk", "shard"), None), P(None, "shard"), P("blk", "shard", None), P())

    return jax.shard_map(body, mesh=mesh, in_specs=in_specs, out_specs=P("blk", "shard", None), check_vma=False)
```

```python
import functools

import jax
import jax.numpy as jnp
from jax import lax
from jax.experimental import pallas as pl
from jax.experimental.pallas import tpu as pltpu
from jax.sharding import PartitionSpec as P


learn_rate = 2.0
AHEAD = 3
LOADED = 2
VMEM_LIMIT = 16 * 1024 * 1024
CUTS = (2, 4, 5, 3, 2)


def shifted(x, axis, by):
    devices = lax.axis_size(axis)
    return lax.ppermute(x, axis, [(i, (i + by) % devices) for i in range(devices)])


def exchanged(blocks, sign):
    workers = len(blocks)
    moved = {}
    for j in sorted(range(1, workers), key=lambda j: abs(2 * j - workers)):
        moved[j] = shifted(blocks[j], "blk", sign * j)
    return [blocks[0]] + [moved[j] for j in range(1, workers)]


def other_core(x):
    devices = lax.axis_size("shard")
    return lax.ppermute(x, "shard", [(i, i ^ 1) for i in range(devices)])


def mix_kernel(rounds, workers, weights_ref, *refs):
    mixed = [ref[...].astype(jnp.float32) for ref in refs[:workers]]
    for r in range(rounds):
        mixed = [
            (
                weights_ref[r, j, 0] * mixed[j]
                + weights_ref[r, j, 1] * mixed[(j + 1) % workers]
                + weights_ref[r, j, 2] * mixed[(j - 1) % workers]
            )
            .astype(jnp.bfloat16)
            .astype(jnp.float32)
            for j in range(workers)
        ]
    total = mixed[0]
    for m in mixed[1:]:
        total = total + m
    average = total * (1.0 / workers)
    for j in range(workers):
        refs[workers + j][...] = (mixed[j] - average).astype(jnp.bfloat16)


def mix_blocks(blocks, weights):
    workers = len(blocks)
    rows, width = blocks[0].shape
    tile = next(t for t in (32, 16, 8) if rows % t == 0)
    spec = pl.BlockSpec((tile, width), lambda i: (i, 0))
    return pl.pallas_call(
        functools.partial(mix_kernel, weights.shape[0], workers),
        grid=(rows // tile,),
        in_specs=[pl.BlockSpec(memory_space=pltpu.SMEM)] + [spec] * workers,
        out_specs=[spec] * workers,
        out_shape=[jax.ShapeDtypeStruct((rows, width), jnp.bfloat16)] * workers,
        cost_estimate=pl.CostEstimate(
            flops=20 * workers * rows * width,
            bytes_accessed=4 * workers * rows * width,
            transcendentals=0,
        ),
        compiler_params=pltpu.CompilerParams(vmem_limit_bytes=VMEM_LIMIT // 2),
        name="mix_blocks",
    )(weights, *blocks)


def place_kernel(begin, *refs):
    blocks, result_ref, sems = refs[: -2], refs[-2], refs[-1]
    workers, _, _ = result_ref.shape
    blocks = blocks[:workers]
    me = lax.axis_index("blk")
    copies = []
    for j in range(workers):
        target = result_ref.at[lax.rem(me + j, workers), :, pl.ds(begin, blocks[j].shape[1])]
        copies.append(pltpu.make_async_copy(blocks[j], target, sems.at[j]))
    for copy in copies:
        copy.start()
    for copy in copies:
        copy.wait()


def place_blocks(blocks, begin, shape, result):
    workers = len(blocks)
    inside = pl.BlockSpec(memory_space=pltpu.VMEM)
    outside = pl.BlockSpec(memory_space=pl.ANY)
    held = [] if result is None else [result]
    return pl.pallas_call(
        functools.partial(place_kernel, begin),
        in_specs=[inside] * workers + [outside] * len(held),
        out_specs=outside,
        out_shape=jax.ShapeDtypeStruct(shape, jnp.bfloat16),
        scratch_shapes=[pltpu.SemaphoreType.DMA((workers,))],
        input_output_aliases={workers: 0} if held else {},
        cost_estimate=pl.CostEstimate(
            flops=4 * blocks[0].size * workers, bytes_accessed=4 * blocks[0].size * workers, transcendentals=0
        ),
        compiler_params=pltpu.CompilerParams(vmem_limit_bytes=VMEM_LIMIT // 2),
        name="place_blocks",
    )(*blocks, *held)


def out_kernel(begin, scale, loaded, *refs):
    if loaded:
        part_ref, own_ref, other_ref = refs[-3:]
        refs = refs[:-3]
    else:
        weight_ref, own_ref, other_ref, part_ref, sem = refs[-5:]
        refs = refs[:-5]
        copy = pltpu.make_async_copy(weight_ref.at[:, pl.ds(begin, own_ref.shape[2])], part_ref, sem)
        copy.start()
        copy.wait()
    chips, _, step = own_ref.shape
    hidden_refs, targets_refs = refs[: 2 * chips], refs[2 * chips :]
    for d in range(chips):
        own, other = (
            jnp.dot(ref[...], part_ref[...], preferred_element_type=jnp.float32) * scale
            for ref in hidden_refs[2 * d : 2 * d + 2]
        )
        if d == 0 and targets_refs:
            own = own - targets_refs[0][:, begin : begin + step].astype(jnp.float32)
        own_ref[d] = own
        other_ref[d] = other.astype(jnp.bfloat16)


def out_part(hidden, targets, weight, begin, step, scale, keep):
    chips, rows = len(hidden) // 2, hidden[0].shape[0]
    inside = pl.BlockSpec(memory_space=pltpu.VMEM)
    outside = pl.BlockSpec(memory_space=pl.ANY)
    units = weight.shape[0]
    loaded = weight.shape[1] == step
    return pl.pallas_call(
        functools.partial(out_kernel, begin, scale, loaded),
        in_specs=[inside] * (2 * chips + len(targets)) + [inside if loaded else outside],
        out_specs=[inside] * (3 if keep else 2),
        out_shape=[
            jax.ShapeDtypeStruct((chips, rows, step), jnp.float32),
            jax.ShapeDtypeStruct((chips, rows, step), jnp.bfloat16),
        ]
        + ([jax.ShapeDtypeStruct((units, step), jnp.bfloat16)] if keep else []),
        scratch_shapes=[]
        if loaded
        else ([] if keep else [pltpu.VMEM((units, step), jnp.bfloat16)]) + [pltpu.SemaphoreType.DMA],
        compiler_params=pltpu.CompilerParams(vmem_limit_bytes=VMEM_LIMIT),
        cost_estimate=pl.CostEstimate(
            flops=4 * chips * rows * units * step, bytes_accessed=2 * units * step, transcendentals=0
        ),
        name="out_part",
    )(*hidden, *targets, weight)


def grad_kernel(begin, scale, chips, unrolled, loaded, *refs):
    hidden_refs, refs = refs[: 2 * chips], refs[2 * chips :]
    resid_ref, other_ref, weight_ref = refs[:3]
    if loaded:
        part_ref = weight_ref
        block_refs, (stepped_ref,) = refs[3:-1], refs[-1:]
    else:
        block_refs, (stepped_ref, part_ref, sem) = refs[3:-3], refs[-3:]
    workers = len(block_refs)
    step = resid_ref.shape[2]
    units = part_ref.shape[0]
    block = units // workers
    tile = next(t for t in (256, 128) if units % t == 0)
    if not loaded:
        copy = pltpu.make_async_copy(weight_ref.at[:, pl.ds(begin, step)], part_ref, sem)
        copy.start()

    def one_tile(i):
        at = pl.ds(i * tile if isinstance(i, int) else pl.multiple_of(i * tile, tile), tile)
        grad = None
        for piece, hidden_ref in enumerate(hidden_refs):
            term = lax.dot_general(
                hidden_ref[:, at],
                (resid_ref, other_ref)[piece % 2][piece // 2],
                (((0,), (0,)), ((), ())),
                preferred_element_type=jnp.float32,
            )
            grad = term if grad is None else grad + term
        if not loaded:
            pl.when(i == 0)(copy.wait)
        stepped_ref[at] = (part_ref[at].astype(jnp.float32) - scale * grad).astype(jnp.bfloat16)

    if unrolled:
        for i in range(units // tile):
            one_tile(i)
    else:
        pl.loop(0, units // tile)(one_tile)
    me = lax.axis_index("blk")
    for j in range(workers):
        first = pl.multiple_of(lax.rem(me + j, workers) * block, 8)
        block_refs[j][...] = stepped_ref[pl.ds(first, block), :]


def grad_part(hidden, resid, other, weight, begin, scale, workers, unrolled):
    chips, rows, step = resid.shape
    units = weight.shape[0]
    loaded = weight.shape[1] == step
    inside = pl.BlockSpec(memory_space=pltpu.VMEM)
    outside = pl.BlockSpec(memory_space=pl.ANY)
    return pl.pallas_call(
        functools.partial(grad_kernel, begin, scale, chips, unrolled, loaded),
        in_specs=[inside] * (2 * chips + 2) + [inside if loaded else outside],
        out_specs=[inside] * workers,
        out_shape=[jax.ShapeDtypeStruct((units // workers, step), jnp.bfloat16)] * workers,
        scratch_shapes=[pltpu.VMEM((units, step), jnp.bfloat16)]
        + ([] if loaded else [pltpu.VMEM((units, step), jnp.bfloat16), pltpu.SemaphoreType.DMA]),
        compiler_params=pltpu.CompilerParams(vmem_limit_bytes=VMEM_LIMIT),
        cost_estimate=pl.CostEstimate(
            flops=4 * chips * rows * units * step, bytes_accessed=4 * units * step, transcendentals=0
        ),
        name="grad_part",
    )(*hidden, resid, other, weight)


def body(tokens, targets, up_weight, down_weight, mix_numer):
    weight = down_weight[0]
    units, width = weight.shape
    workers = lax.axis_size("blk")
    me = lax.axis_index("blk")
    shards = lax.axis_size("shard")
    chips = shards // 2
    block = units // workers
    out_scale = 1.0 / (units * shards) ** 0.5
    parts = len(CUTS)

    mine = [tokens] + [shifted(tokens, "shard", -2 * d) for d in range(1, chips)]
    hidden = []
    for x in mine:
        pair = (x, other_core(x))
        for x in pair:
            hidden.append(jax.nn.silu(jnp.dot(x, up_weight, preferred_element_type=jnp.float32)).astype(jnp.bfloat16))

    order = (me - jnp.arange(workers)) % workers
    weights = jnp.take(mix_numer, order, axis=1).astype(jnp.float32) * 0.25

    unit = width // sum(CUTS)
    begins = [unit * sum(CUTS[:c]) for c in range(parts)]
    arrived = []
    for c in range(parts):
        step = unit * CUTS[c]
        source = weight
        runs = ((0, 1), (1, chips)) if c < AHEAD and chips > 1 else ((0, chips),)
        sums = []
        got = {}
        for first, last in runs:
            keep = c < LOADED and source is weight
            own, other, *part = out_part(
                hidden[2 * first : 2 * last],
                [] if first else [targets],
                source,
                begins[c],
                step,
                out_scale,
                keep,
            )
            if keep:
                source = part[0]
            if sums:
                own, *sums = lax.optimization_barrier((own, *sums))
            summed = (own + other_core(other).astype(jnp.float32)).astype(jnp.bfloat16)
            sums += [summed[i] for i in range(last - first)]
            if c and last < chips:
                continue
            sent = summed if c == 0 or len(runs) == 1 else jnp.stack(sums)
            for d in range(1, chips):
                moved = shifted(sent, "shard", -2 * d)
                for i in range(sent.shape[0]):
                    got.setdefault((d + i + (first if c == 0 else 0)) % chips, []).append(moved[i])
        totals = [x.astype(jnp.float32) for x in sums]
        for n, terms in got.items():
            for x in terms:
                totals[n] = totals[n] + x.astype(jnp.float32)
        resid = jnp.stack(totals).astype(jnp.bfloat16)
        other = other_core(resid)
        blocks = grad_part(hidden, resid, other, source, begins[c], learn_rate * out_scale, workers, c < 2)
        arrived.append(exchanged(blocks, 1))
    returned = []
    for c in range(parts):
        drift = mix_blocks(arrived[c], weights)
        returned.append(exchanged(drift, -1))
    result = None
    for c in range(parts):
        result = place_blocks(returned[c], begins[c], (workers, block, width), result)
    return result.reshape(1, units, width)


def solution(mesh):
    in_specs = (P(("blk", "shard"), None), P(("blk", "shard"), None), P(None, "shard"), P("blk", "shard", None), P())

    return jax.shard_map(body, mesh=mesh, in_specs=in_specs, out_specs=P("blk", "shard", None), check_vma=False)
```
